32 devices in a mesh: dp: 2 (over x), sp: 16 (over y, z, core).
Axes of the slice: x: 2, y: 2, z: 4, core: 2. Of those that a mesh axis runs over, the one named last changes fastest.
Arguments:
- x: bfloat16 [4096, 12288], P(('dp', 'sp')), parts along dimension 0
- gain: bfloat16 [12288], replicated
- wq: bfloat16 [12288, 12288], replicated
- wk: bfloat16 [12288, 12288], replicated
- wv: bfloat16 [12288, 12288], replicated
- wo: bfloat16 [12288, 12288], replicated
Outputs:
- output: bfloat16 [4096, 12288], P(('dp', 'sp')), parts along dimension 0
There are 2 independent parts. The reference program is written for one: setup_inputs(seed, part) draws one part's arguments, and reference() takes and returns one part's arrays. A program takes and returns all parts, laid end to end along the dimension named above; an argument that names none is the same for every part.
All inputs are finite; a program needn't handle non-finite values.
Results may differ from the reference program's by a relative error of at most 0.012.
Values are sent between devices in bfloat16 or wider.
A program may use at most 2.75 GiB of HBM per device.

```python
import jax
import jax.numpy as jnp
from jax import lax

ROWS = 2048
D = 12288
HEADS = 96
KV_HEADS = 96
HEAD = 128
THETA = 10000


def setup_inputs(seed: int = 0, part: int = 0) -> dict:
    kx, kn, kq, kk, kv, ko = jax.random.split(jax.random.key(seed), 6)

    def weights(key, rows, columns):
        return jax.random.normal(key, (rows, columns), jnp.float32) * rows**-0.5

    drawn = {
        "x": jax.random.normal(jax.random.fold_in(kx, part), (ROWS, D), jnp.float32),
        "gain": 1 + 0.1 * jax.random.normal(kn, (D,), jnp.float32),
        "wq": 2 * weights(kq, D, HEADS * HEAD),
        "wk": 2 * weights(kk, D, KV_HEADS * HEAD),
        "wv": 4 * weights(kv, D, KV_HEADS * HEAD),
        "wo": weights(ko, HEADS * HEAD, D),
    }
    return {k: v.astype(jnp.bfloat16) for k, v in drawn.items()}


def normed(x, gain):
    wide = x.astype(jnp.float32)
    scale = lax.rsqrt(jnp.mean(wide * wide, -1, keepdims=True) + 1e-6)
    return (wide * scale * gain.astype(jnp.float32)).astype(jnp.bfloat16)


def turned(t, place, theta):
    half = t.shape[-1] // 2
    angle = place.astype(jnp.float32)[:, None] * theta ** (-jnp.arange(half, dtype=jnp.float32) / half)
    cos, sin = jnp.cos(angle)[:, None], jnp.sin(angle)[:, None]
    a, b = t[..., :half].astype(jnp.float32), t[..., half:].astype(jnp.float32)
    return jnp.concatenate([a * cos - b * sin, b * cos + a * sin], -1).astype(jnp.bfloat16)


def matmul(a, w):
    return jnp.dot(a, w, preferred_element_type=jnp.float32).astype(jnp.bfloat16)


def einsum(form, a, b):
    return jnp.einsum(form, a.astype(jnp.float32), b.astype(jnp.float32))


def attention(q, k, v):
    scores = einsum("tgsd,ugd->gstu", q, k) * q.shape[-1] ** -0.5
    token = jnp.arange(q.shape[0])
    scores = jnp.where(token[:, None] >= token, scores, -jnp.inf)
    weights = jax.nn.softmax(scores, -1).astype(jnp.bfloat16)
    return einsum("gstu,ugd->tgsd", weights, v).astype(jnp.bfloat16)


def reference(x, gain, wq, wk, wv, wo):
    a, place = normed(x, gain), jnp.arange(ROWS)
    q = turned(matmul(a, wq).reshape(ROWS, HEADS, HEAD), place, THETA).reshape(ROWS, KV_HEADS, -1, HEAD)
    k = turned(matmul(a, wk).reshape(ROWS, KV_HEADS, HEAD), place, THETA)
    v = matmul(a, wv).reshape(ROWS, KV_HEADS, HEAD)
    seen = attention(q, k, v).reshape(ROWS, HEADS * HEAD)
    return (x.astype(jnp.float32) + jnp.dot(seen, wo, preferred_element_type=jnp.float32)).astype(jnp.bfloat16)
```

```python
import jax
import jax.numpy as jnp
from jax import lax
from jax.experimental import pallas as pl
from jax.experimental.pallas import tpu as pltpu

NEG = -1e30
HIDDEN = 2 * NEG
LOG2E = 1.4426950408889634


def _dot(a, b, ca, cb):
    return lax.dot_general(a, b, (((ca,), (cb,)), ((), ())), preferred_element_type=jnp.float32)


from jax.sharding import PartitionSpec as P

HEAD = 128
THETA = 10000
CHIPS = 8
OWN = 4
ROUNDS = 3 * CHIPS
KQ, QUARTERS, SLOTS = 3072, 4, 6
BLOCK = 512
MESH = pl.DeviceIdType.MESH


def _step(x_ref, gain_ref, cos_ref, sin_ref, wq_ref, wk_ref, wv_ref, wo_ref, y_ref, a_s, w_s, stage, recv, sstage, srecv, acc, exch, mix_s,
          top_s, w_sem, x_sem, y_sem, a_send, a_recv, t_send, t_recv, s_send, s_recv, e_send, e_recv):
    me = lax.axis_index("sp")
    s, c = me // 2, me % 2
    row, col = s // 4, s % 4
    own, chip_rows = x_ref.shape[0], 2 * x_ref.shape[0]
    mine = pl.multiple_of(c * own, own)
    theirs = pl.multiple_of((1 - c) * own, own)
    my_tokens = pl.ds(pl.multiple_of(s * chip_rows, chip_rows), chip_rows)

    def there(chip, core):
        return {"sp": chip * 2 + core}

    def peer(r):
        return lax.rem(row + lax.rem(r, 2), 2) * 4 + lax.rem(col + 2 + r // 2, 4)

    def weights(i, at):
        src = (wq_ref, wk_ref, wv_ref)[at // QUARTERS]
        pair = c * ROUNDS + (i // CHIPS) * CHIPS + peer(lax.rem(i, CHIPS))
        return pltpu.make_async_copy(
            src.at[pl.ds((at % QUARTERS) * KQ, KQ), pl.ds(pl.multiple_of(pair * 256, 256), 256)], w_s.at[at % SLOTS], w_sem.at[at % SLOTS])

    load = pltpu.make_async_copy(x_ref, a_s.at[pl.ds(mine, own)], x_sem)
    load.start()
    for at in range(SLOTS):
        weights(0, at).start()

    barrier = pltpu.get_barrier_semaphore()
    for r in range(1, CHIPS):
        pl.semaphore_signal(barrier, inc=1, device_id=there(lax.rem(s + r, CHIPS), c), device_id_type=MESH)
    pl.semaphore_signal(barrier, inc=1, device_id=there(s, 1 - c), device_id_type=MESH)
    pl.semaphore_wait(barrier, CHIPS)
    load.wait()

    shares = []
    for p in range(4):
        def norm(g, _):
            rows = pl.ds(pl.multiple_of(mine + p * 32 + g * 16, 16), 16)
            wide = a_s[rows, :].astype(jnp.float32)
            scale = lax.rsqrt(jnp.mean(wide * wide, -1, keepdims=True) + 1e-6)
            a_s[rows, :] = (wide * scale * gain_ref[...]).astype(jnp.bfloat16)

        lax.fori_loop(0, 2, norm, None)
        rows = pl.ds(pl.multiple_of(mine + p * 32, 32), 32)
        shares.append(pltpu.make_async_remote_copy(a_s.at[rows], a_s.at[rows], a_send.at[p], a_recv.at[p], device_id=there(s, 1 - c),
                                                   device_id_type=MESH))
        shares[-1].start()
    for share in shares:
        share.wait()

    def tile_copy(i, kind):
        return pltpu.make_async_remote_copy(
            stage.at[lax.rem(i, 16), kind], recv.at[i // CHIPS, kind, :, my_tokens, :], t_send.at[i, kind], t_recv.at[i, kind],
            device_id=there(peer(lax.rem(i, CHIPS)), c), device_id_type=MESH)

    def tiles(i, _):
        j, r = i // CHIPS, lax.rem(i, CHIPS)
        for kind in range(3):
            total = None
            for part in range(QUARTERS):
                at = kind * QUARTERS + part
                weights(i, at).wait()
                term = _dot(a_s[:, part * KQ : (part + 1) * KQ], w_s[at % SLOTS], 1, 0)
                total = term if total is None else total + term
                if at + SLOTS < 3 * QUARTERS:
                    weights(i, at + SLOTS).start()
                else:
                    @pl.when(i + 1 < ROUNDS)
                    def _():
                        weights(i + 1, at + SLOTS - 3 * QUARTERS).start()
            total = total.astype(jnp.bfloat16)
            heads = [total[:, :HEAD], total[:, HEAD:]]
            if kind < 2:
                wide = [h.astype(jnp.float32) for h in heads]
                heads = [(h * cos_ref[...] + pltpu.roll(h, HEAD // 2, 1) * sin_ref[...]).astype(jnp.bfloat16) for h in wide]

            @pl.when(r == OWN)
            def _():
                for n, h in enumerate(heads):
                    recv[j, kind, n, my_tokens, :] = h

            @pl.when(r != OWN)
            def _():
                @pl.when(i >= 16)
                def _():
                    tile_copy(i - 16, kind).wait_send()

                for n, h in enumerate(heads):
                    stage[lax.rem(i, 16), kind, n] = h
                tile_copy(i, kind).start()

    lax.fori_loop(0, ROUNDS, tiles, None)

    def out_weights(u):
        rows = pl.ds(pl.multiple_of((c * ROUNDS + (u // 48) * CHIPS) * 256, 2048), 2048)
        return pltpu.make_async_copy(wo_ref.at[rows, pl.ds(pl.multiple_of(lax.rem(u, 48) * 256, 256), 256)],
                                     w_s.at[lax.rem(u, SLOTS), pl.ds(0, 2048)], w_sem.at[lax.rem(u, SLOTS)])

    for u in range(SLOTS):
        out_weights(u).start()
    again = pltpu.make_async_copy(x_ref, a_s.at[pl.ds(0, own)], x_sem)
    again.start()

    e = HEAD**-0.5 * LOG2E
    pieces = [(n, h) for n in range(2) for h in range(2)]

    def seen_copy(j, chip):
        return pltpu.make_async_remote_copy(
            sstage.at[j, chip], srecv.at[j, :, my_tokens_of(s)], s_send.at[j, chip], s_recv.at[j, s], device_id=there(chip, c),
            device_id_type=MESH)

    def my_tokens_of(chip):
        return pl.ds(pl.multiple_of(chip * 256, 256), 256)

    def attention(j, _):
        def arrived(r, _):
            @pl.when(r != OWN)
            def _():
                for kind in range(3):
                    tile_copy(j * CHIPS + r, kind).wait_recv()

        lax.fori_loop(0, CHIPS, arrived, None)
        ones = jnp.ones((8, BLOCK), jnp.bfloat16)

        def queries(b, _):
            for m in range(4):
                top_s[m : m + 1, :] = jnp.full((1, BLOCK), NEG, jnp.float32)
                mix_s[m] = jnp.zeros((HEAD + 8, BLOCK), jnp.float32)

            def block(k, whole, cut):
                here = pl.ds(pl.multiple_of(k * BLOCK, BLOCK), BLOCK)
                strips = [m for m in range(4) if m in whole or m in cut]
                scores = [_dot(recv[j, 1, pieces[m][0], here, :],
                               recv[j, 0, pieces[m][0], pl.ds(pl.multiple_of((b * 2 + pieces[m][1]) * BLOCK, BLOCK), BLOCK), :], 1, 1)
                          for m in strips]
                if cut:
                    ok = lax.broadcasted_iota(jnp.int32, (BLOCK, BLOCK), 1) >= lax.broadcasted_iota(jnp.int32, (BLOCK, BLOCK), 0)
                ps, keeps = [], []
                for m, score in zip(strips, scores):
                    if m in cut:
                        score = jnp.where(ok, score, HIDDEN)
                    old = top_s[m : m + 1, :]
                    top = jnp.maximum(old, score.max(axis=0, keepdims=True))
                    top_s[m : m + 1, :] = top
                    ps.append(jnp.exp2((score - top) * e).astype(jnp.bfloat16))
                    keeps.append(jnp.exp2((old - top) * e))
                for m, p, keep in zip(strips, ps, keeps):
                    values = jnp.concatenate([recv[j, 2, pieces[m][0], here, :].T, ones], axis=0)
                    mix_s[m] = mix_s[m] * keep + _dot(values, p, 1, 0)

            lax.fori_loop(0, b * 2, lambda k, _: block(k, (0, 1, 2, 3), ()), None)
            block(b * 2, (1, 3), (0, 2))
            block(b * 2 + 1, (), (1, 3))
            for m, (n, h) in enumerate(pieces):
                out = (mix_s[m, :HEAD, :] * (1 / mix_s[m, HEAD : HEAD + 1, :])).T.astype(jnp.bfloat16)
                for q in range(2):
                    chip = b * 4 + h * 2 + q
                    piece = out[q * 256 : (q + 1) * 256]

                    @pl.when(chip == s)
                    def _():
                        srecv[j, :, pl.ds(pl.multiple_of(s * 256 + n * HEAD, HEAD), HEAD)] = piece

                    @pl.when(chip != s)
                    def _():
                        sstage[j, chip, :, n * HEAD : (n + 1) * HEAD] = piece

            def send(q, _):
                @pl.when(b * 4 + q != s)
                def _():
                    seen_copy(j, b * 4 + q).start()

            lax.fori_loop(0, 4, send, None)

        lax.fori_loop(0, 2, queries, None)

    lax.fori_loop(0, 3, attention, None)

    again.wait()

    def sum_copy(n):
        return pltpu.make_async_remote_copy(acc.at[n, pl.ds(theirs, own)], exch.at[n], e_send.at[n], e_recv.at[n],
                                            device_id=there(s, 1 - c), device_id_type=MESH)

    def columns(n):
        return pl.ds(pl.multiple_of(n * 256, 256), 256)

    def y_copy(n):
        return pltpu.make_async_copy(a_s.at[pl.ds(own, own), columns(n)], y_ref.at[:, columns(n)], y_sem)

    def finish(n):
        sum_copy(n).wait_recv()
        y = a_s[pl.ds(0, own), columns(n)].astype(jnp.float32) + (acc[n, pl.ds(mine, own), :] + exch[n])
        a_s[pl.ds(own, own), columns(n)] = y.astype(jnp.bfloat16)
        y_copy(n).start()

    for j in range(3):
        def here(chip, _):
            @pl.when(chip != s)
            def _():
                pltpu.make_async_remote_copy(sstage.at[j, chip], srecv.at[j, :, my_tokens_of(chip)], s_send.at[j, chip], s_recv.at[j, chip],
                                             device_id=there(chip, c), device_id_type=MESH).wait_recv()

        lax.fori_loop(0, CHIPS, here, None)

        def project(n, _):
            u = j * 48 + n
            out_weights(u).wait()
            term = _dot(srecv[j], w_s[lax.rem(u, SLOTS), :2048, :], 1, 0)

            @pl.when(u + SLOTS < 144)
            def _():
                out_weights(u + SLOTS).start()

            acc[n] = term if j == 0 else acc[n] + term
            if j == 2:
                sum_copy(n).start()

                @pl.when(n >= 4)
                def _():
                    finish(n - 4)

        lax.fori_loop(0, 48, project, None)
    for n in range(44, 48):
        finish(n)

    def sent(i, _):
        @pl.when(lax.rem(i, CHIPS) != OWN)
        def _():
            for kind in range(3):
                tile_copy(i, kind).wait_send()

    lax.fori_loop(8, ROUNDS, sent, None)

    def seen_sent(i, _):
        @pl.when(lax.rem(i, CHIPS) != s)
        def _():
            seen_copy(i // CHIPS, lax.rem(i, CHIPS)).wait_send()

    lax.fori_loop(0, ROUNDS, seen_sent, None)
    lax.fori_loop(0, 48, lambda n, _: sum_copy(n).wait_send(), None)
    pltpu.make_async_copy(a_s.at[pl.ds(own, own)], y_ref, y_sem).wait()


def solution(mesh):
    def step(x, gain, wq, wk, wv, wo):
        own, d = x.shape
        half = HEAD // 2
        place = lax.axis_index("sp") // 2 * (2 * own) + jnp.arange(2 * own)
        angle = place.astype(jnp.float32)[:, None] * THETA ** (-jnp.arange(half, dtype=jnp.float32) / half)
        cos, sin = jnp.cos(angle), jnp.sin(angle)
        vmem, hbm = pl.BlockSpec(memory_space=pltpu.VMEM), pl.BlockSpec(memory_space=pltpu.HBM)
        bf16, f32, dma = jnp.bfloat16, jnp.float32, pltpu.SemaphoreType.DMA
        return pl.pallas_call(
            _step,
            out_shape=jax.ShapeDtypeStruct((own, d), bf16),
            in_specs=[hbm, vmem, vmem, vmem, hbm, hbm, hbm, hbm],
            out_specs=hbm,
            scratch_shapes=[
                pltpu.VMEM((2 * own, d), bf16),
                pltpu.VMEM((SLOTS, KQ, 256), bf16),
                pltpu.VMEM((16, 3, 2, 2 * own, HEAD), bf16),
                pltpu.VMEM((3, 3, 2, 16 * own, HEAD), bf16),
                pltpu.VMEM((3, CHIPS, 2 * own, 256), bf16),
                pltpu.VMEM((3, 2 * own, 2048), bf16),
                pltpu.VMEM((48, 2 * own, 256), f32),
                pltpu.VMEM((48, own, 256), f32),
                pltpu.VMEM((4, HEAD + 8, BLOCK), f32),
                pltpu.VMEM((8, BLOCK), f32),
                dma((SLOTS,)), dma, dma, dma((4,)), dma((4,)), dma((ROUNDS, 3)), dma((ROUNDS, 3)),
                dma((3, CHIPS)), dma((3, CHIPS)), dma((48,)), dma((48,)),
            ],
            compiler_params=pltpu.CompilerParams(collective_id=0, has_side_effects=True, vmem_limit_bytes=67043328),
        )(x, gain.astype(f32)[None], jnp.concatenate([cos, cos], -1), jnp.concatenate([-sin, sin], -1), wq, wk, wv, wo)

    tokens, whole = P(("dp", "sp"), None), P(None, None)
    return jax.shard_map(
        step,
        mesh=mesh,
        in_specs=(tokens, P(None), whole, whole, whole, whole),
        out_specs=tokens,
        check_vma=False,
    )
```

```python
import jax
import jax.numpy as jnp
from jax import lax
from jax.experimental import pallas as pl
from jax.experimental.pallas import tpu as pltpu

NEG = -1e30
HIDDEN = 2 * NEG
LOG2E = 1.4426950408889634


def _dot(a, b, ca, cb):
    return lax.dot_general(a, b, (((ca,), (cb,)), ((), ())), preferred_element_type=jnp.float32)


from jax.sharding import PartitionSpec as P

HEAD = 128
THETA = 10000
CHIPS = 8
OWN = 4
ROUNDS = 3 * CHIPS
KQ, QUARTERS, SLOTS = 3072, 4, 6
BLOCK = 512
MESH = pl.DeviceIdType.MESH


def _step(x_ref, gain_ref, cos_ref, sin_ref, wq_ref, wk_ref, wv_ref, wo_ref, y_ref, a_s, w_s, stage, recv, sstage, srecv, acc, exch, mix_s,
          top_s, w_sem, x_sem, y_sem, a_send, a_recv, t_send, t_recv, s_send, s_recv, e_send, e_recv):
    me = lax.axis_index("sp")
    s, c = me // 2, me % 2
    row, col = s // 4, s % 4
    own, chip_rows = x_ref.shape[0], 2 * x_ref.shape[0]
    mine = pl.multiple_of(c * own, own)
    theirs = pl.multiple_of((1 - c) * own, own)
    my_tokens = pl.ds(pl.multiple_of(s * chip_rows, chip_rows), chip_rows)

    def there(chip, core):
        return {"sp": chip * 2 + core}

    def peer(r):
        return lax.rem(row + lax.rem(r, 2), 2) * 4 + lax.rem(col + 2 + r // 2, 4)

    def weights(i, at):
        src = (wq_ref, wk_ref, wv_ref)[at // QUARTERS]
        pair = c * ROUNDS + (i // CHIPS) * CHIPS + peer(lax.rem(i, CHIPS))
        return pltpu.make_async_copy(
            src.at[pl.ds((at % QUARTERS) * KQ, KQ), pl.ds(pl.multiple_of(pair * 256, 256), 256)], w_s.at[at % SLOTS], w_sem.at[at % SLOTS])

    load = pltpu.make_async_copy(x_ref, a_s.at[pl.ds(mine, own)], x_sem)
    load.start()
    for at in range(SLOTS):
        weights(0, at).start()

    barrier = pltpu.get_barrier_semaphore()
    for r in range(1, CHIPS):
        pl.semaphore_signal(barrier, inc=1, device_id=there(lax.rem(s + r, CHIPS), c), device_id_type=MESH)
    pl.semaphore_signal(barrier, inc=1, device_id=there(s, 1 - c), device_id_type=MESH)
    pl.semaphore_wait(barrier, CHIPS)
    load.wait()

    shares = []
    for p in range(4):
        def norm(g, _):
            rows = pl.ds(pl.multiple_of(mine + p * 32 + g * 16, 16), 16)
            wide = a_s[rows, :].astype(jnp.float32)
            scale = lax.rsqrt(jnp.mean(wide * wide, -1, keepdims=True) + 1e-6)
            a_s[rows, :] = (wide * scale * gain_ref[...]).astype(jnp.bfloat16)

        lax.fori_loop(0, 2, norm, None)
        rows = pl.ds(pl.multiple_of(mine + p * 32, 32), 32)
        shares.append(pltpu.make_async_remote_copy(a_s.at[rows], a_s.at[rows], a_send.at[p], a_recv.at[p], device_id=there(s, 1 - c),
                                                   device_id_type=MESH))
        shares[-1].start()
    for share in shares:
        share.wait()

    def tile_copy(i):
        return pltpu.make_async_remote_copy(
            stage.at[lax.rem(i, 16)], recv.at[i // CHIPS, :, my_tokens, :], t_send.at[i], t_recv.at[i],
            device_id=there(peer(lax.rem(i, CHIPS)), c), device_id_type=MESH)

    def tiles(i, _):
        j, r = i // CHIPS, lax.rem(i, CHIPS)

        @pl.when((r != OWN) & (i >= 16))
        def _():
            tile_copy(i - 16).wait_send()

        for kind in range(3):
            total = None
            for part in range(QUARTERS):
                at = kind * QUARTERS + part
                weights(i, at).wait()
                term = _dot(a_s[:, part * KQ : (part + 1) * KQ], w_s[at % SLOTS], 1, 0)
                total = term if total is None else total + term
                if at + SLOTS < 3 * QUARTERS:
                    weights(i, at + SLOTS).start()
                else:
                    @pl.when(i + 1 < ROUNDS)
                    def _():
                        weights(i + 1, at + SLOTS - 3 * QUARTERS).start()
            total = total.astype(jnp.bfloat16)
            heads = [total[:, :HEAD], total[:, HEAD:]]
            if kind < 2:
                wide = [h.astype(jnp.float32) for h in heads]
                heads = [(h * cos_ref[...] + pltpu.roll(h, HEAD // 2, 1) * sin_ref[...]).astype(jnp.bfloat16) for h in wide]

            @pl.when(r == OWN)
            def _():
                for n, h in enumerate(heads):
                    recv[j, kind * 2 + n, my_tokens, :] = h

            @pl.when(r != OWN)
            def _():
                for n, h in enumerate(heads):
                    stage[lax.rem(i, 16), kind * 2 + n] = h

        @pl.when(r != OWN)
        def _():
            tile_copy(i).start()

    lax.fori_loop(0, ROUNDS, tiles, None)

    def out_weights(u):
        rows = pl.ds(pl.multiple_of((c * ROUNDS + (u // 48) * CHIPS) * 256, 2048), 2048)
        return pltpu.make_async_copy(wo_ref.at[rows, pl.ds(pl.multiple_of(lax.rem(u, 48) * 256, 256), 256)],
                                     w_s.at[lax.rem(u, SLOTS), pl.ds(0, 2048)], w_sem.at[lax.rem(u, SLOTS)])

    for u in range(SLOTS):
        out_weights(u).start()
    again = pltpu.make_async_copy(x_ref, a_s.at[pl.ds(0, own)], x_sem)
    again.start()

    e = HEAD**-0.5 * LOG2E
    pieces = [(n, h) for n in range(2) for h in range(2)]

    def seen_copy(j, chip):
        return pltpu.make_async_remote_copy(
            sstage.at[j, chip], srecv.at[j, :, my_tokens_of(s)], s_send.at[j, chip], s_recv.at[j, s], device_id=there(chip, c),
            device_id_type=MESH)

    def my_tokens_of(chip):
        return pl.ds(pl.multiple_of(chip * 256, 256), 256)

    def attention(j, _):
        def arrived(r, _):
            @pl.when(r != OWN)
            def _():
                tile_copy(j * CHIPS + r).wait_recv()

        lax.fori_loop(0, CHIPS, arrived, None)
        ones = jnp.ones((8, BLOCK), jnp.bfloat16)

        def queries(b, _):
            for m in range(4):
                top_s[m : m + 1, :] = jnp.full((1, BLOCK), NEG, jnp.float32)
                mix_s[m] = jnp.zeros((HEAD + 8, BLOCK), jnp.float32)

            def block(k, whole, cut):
                here = pl.ds(pl.multiple_of(k * BLOCK, BLOCK), BLOCK)
                strips = [m for m in range(4) if m in whole or m in cut]
                scores = [_dot(recv[j, 2 + pieces[m][0], here, :],
                               recv[j, pieces[m][0], pl.ds(pl.multiple_of((b * 2 + pieces[m][1]) * BLOCK, BLOCK), BLOCK), :], 1, 1)
                          for m in strips]
                if cut:
                    ok = lax.broadcasted_iota(jnp.int32, (BLOCK, BLOCK), 1) >= lax.broadcasted_iota(jnp.int32, (BLOCK, BLOCK), 0)
                ps, keeps = [], []
                for m, score in zip(strips, scores):
                    if m in cut:
                        score = jnp.where(ok, score, HIDDEN)
                    old = top_s[m : m + 1, :]
                    top = jnp.maximum(old, score.max(axis=0, keepdims=True))
                    top_s[m : m + 1, :] = top
                    ps.append(jnp.exp2((score - top) * e).astype(jnp.bfloat16))
                    keeps.append(jnp.exp2((old - top) * e))
                for m, p, keep in zip(strips, ps, keeps):
                    values = jnp.concatenate([recv[j, 4 + pieces[m][0], here, :].T, ones], axis=0)
                    mix_s[m] = mix_s[m] * keep + _dot(values, p, 1, 0)

            lax.fori_loop(0, b * 2, lambda k, _: block(k, (0, 1, 2, 3), ()), None)
            block(b * 2, (1, 3), (0, 2))
            block(b * 2 + 1, (), (1, 3))
            for m, (n, h) in enumerate(pieces):
                out = (mix_s[m, :HEAD, :] * (1 / mix_s[m, HEAD : HEAD + 1, :])).T.astype(jnp.bfloat16)
                for q in range(2):
                    chip = b * 4 + h * 2 + q
                    piece = out[q * 256 : (q + 1) * 256]

                    @pl.when(chip == s)
                    def _():
                        srecv[j, :, pl.ds(pl.multiple_of(s * 256 + n * HEAD, HEAD), HEAD)] = piece

                    @pl.when(chip != s)
                    def _():
                        sstage[j, chip, :, n * HEAD : (n + 1) * HEAD] = piece

            def send(q, _):
                @pl.when(b * 4 + q != s)
                def _():
                    seen_copy(j, b * 4 + q).start()

            lax.fori_loop(0, 4, send, None)

        lax.fori_loop(0, 2, queries, None)

    lax.fori_loop(0, 3, attention, None)

    again.wait()

    def sum_copy(n):
        return pltpu.make_async_remote_copy(acc.at[n, pl.ds(theirs, own)], exch.at[n], e_send.at[n], e_recv.at[n],
                                            device_id=there(s, 1 - c), device_id_type=MESH)

    def columns(n):
        return pl.ds(pl.multiple_of(n * 256, 256), 256)

    def y_copy(n):
        return pltpu.make_async_copy(a_s.at[pl.ds(own, own), columns(n)], y_ref.at[:, columns(n)], y_sem)

    def finish(n):
        sum_copy(n).wait_recv()
        y = a_s[pl.ds(0, own), columns(n)].astype(jnp.float32) + (acc[n, pl.ds(mine, own), :] + exch[n])
        a_s[pl.ds(own, own), columns(n)] = y.astype(jnp.bfloat16)
        y_copy(n).start()

    for j in range(3):
        def here(chip, _):
            @pl.when(chip != s)
            def _():
                pltpu.make_async_remote_copy(sstage.at[j, chip], srecv.at[j, :, my_tokens_of(chip)], s_send.at[j, chip], s_recv.at[j, chip],
                                             device_id=there(chip, c), device_id_type=MESH).wait_recv()

        lax.fori_loop(0, CHIPS, here, None)

        def project(n, _):
            u = j * 48 + n
            out_weights(u).wait()
            term = _dot(srecv[j], w_s[lax.rem(u, SLOTS), :2048, :], 1, 0)

            @pl.when(u + SLOTS < 144)
            def _():
                out_weights(u + SLOTS).start()

            acc[n] = term if j == 0 else acc[n] + term
            if j == 2:
                sum_copy(n).start()

                @pl.when(n >= 4)
                def _():
                    finish(n - 4)

        lax.fori_loop(0, 48, project, None)
    for n in range(44, 48):
        finish(n)

    def sent(i, _):
        @pl.when(lax.rem(i, CHIPS) != OWN)
        def _():
            tile_copy(i).wait_send()

    lax.fori_loop(8, ROUNDS, sent, None)

    def seen_sent(i, _):
        @pl.when(lax.rem(i, CHIPS) != s)
        def _():
            seen_copy(i // CHIPS, lax.rem(i, CHIPS)).wait_send()

    lax.fori_loop(0, ROUNDS, seen_sent, None)
    lax.fori_loop(0, 48, lambda n, _: sum_copy(n).wait_send(), None)
    pltpu.make_async_copy(a_s.at[pl.ds(own, own)], y_ref, y_sem).wait()


def solution(mesh):
    def step(x, gain, wq, wk, wv, wo):
        own, d = x.shape
        half = HEAD // 2
        place = lax.axis_index("sp") // 2 * (2 * own) + jnp.arange(2 * own)
        angle = place.astype(jnp.float32)[:, None] * THETA ** (-jnp.arange(half, dtype=jnp.float32) / half)
        cos, sin = jnp.cos(angle), jnp.sin(angle)
        vmem, hbm = pl.BlockSpec(memory_space=pltpu.VMEM), pl.BlockSpec(memory_space=pltpu.HBM)
        bf16, f32, dma = jnp.bfloat16, jnp.float32, pltpu.SemaphoreType.DMA
        return pl.pallas_call(
            _step,
            out_shape=jax.ShapeDtypeStruct((own, d), bf16),
            in_specs=[hbm, vmem, vmem, vmem, hbm, hbm, hbm, hbm],
            out_specs=hbm,
            scratch_shapes=[
                pltpu.VMEM((2 * own, d), bf16),
                pltpu.VMEM((SLOTS, KQ, 256), bf16),
                pltpu.VMEM((16, 6, 2 * own, HEAD), bf16),
                pltpu.VMEM((3, 6, 16 * own, HEAD), bf16),
                pltpu.VMEM((3, CHIPS, 2 * own, 256), bf16),
                pltpu.VMEM((3, 2 * own, 2048), bf16),
                pltpu.VMEM((48, 2 * own, 256), f32),
                pltpu.VMEM((48, own, 256), f32),
                pltpu.VMEM((4, HEAD + 8, BLOCK), f32),
                pltpu.VMEM((8, BLOCK), f32),
                dma((SLOTS,)), dma, dma, dma((4,)), dma((4,)), dma((ROUNDS,)), dma((ROUNDS,)),
                dma((3, CHIPS)), dma((3, CHIPS)), dma((48,)), dma((48,)),
            ],
            compiler_params=pltpu.CompilerParams(collective_id=0, has_side_effects=True, vmem_limit_bytes=67043328),
        )(x, gain.astype(f32)[None], jnp.concatenate([cos, cos], -1), jnp.concatenate([-sin, sin], -1), wq, wk, wv, wo)

    tokens, whole = P(("dp", "sp"), None), P(None, None)
    return jax.shard_map(
        step,
        mesh=mesh,
        in_specs=(tokens, P(None), whole, whole, whole, whole),
        out_specs=tokens,
        check_vma=False,
    )
```
